128 devices in a mesh: grp: 4 (over y, x), seq: 32 (over z, core).
Axes of the slice: x: 2, y: 2, z: 16, core: 2. Of those that a mesh axis runs over, the one named last changes fastest.
The devices are a block of a 8x8x16 slice.
Arguments:
- queries: bfloat16 [2048, 4096], P(('grp', 'seq')), parts along dimension 0, may hold values from -36 to 36
- new_keys: bfloat16 [2048, 1024], P(('grp', 'seq')), parts along dimension 0, may hold values from -24 to 24
- new_values: bfloat16 [2048, 1024], P(('grp', 'seq')), parts along dimension 0, may hold values from -12 to 12
- suffix_keys: bfloat16 [2048, 256, 1024], P(('grp', 'seq')), parts along dimension 0, may hold values from -18 to 18
- suffix_values: bfloat16 [2048, 256, 1024], P(('grp', 'seq')), parts along dimension 0, may hold values from -12 to 12
- suffix_lens: int32 [2048], P(('grp', 'seq')), parts along dimension 0, may hold values from 1 to 256, 65536 in all
- prefix_keys: bfloat16 [8192, 16, 1024], P(('grp', 'seq')), parts along dimension 0, may hold values from -12 to 12
- prefix_values: bfloat16 [8192, 16, 1024], P(('grp', 'seq')), parts along dimension 0, may hold values from -12 to 12
- page_table: int32 [8, 1024], P('grp'), parts along dimension 0, may hold values from 0 to 2047, as said below
- prefix_id: int32 [2048], P('grp'), parts along dimension 0, may hold values from 0 to 1
Outputs:
- attn_out: bfloat16 [2048, 4096], P(('grp', 'seq')), parts along dimension 0
The draws below stay inside these ranges and needn't reach their ends.
There are 4 independent parts, one for each index of `grp`. The reference program is written for one: setup_inputs(seed, part) draws one part's arguments, and reference() takes and returns one part's arrays. A program takes and returns all parts, laid end to end along the dimension named above; each array names one. Nothing has to cross between parts.
Inputs may be any that keep to these rules, and one draw needn't show every extreme that they name: `page_table`: every page id 0 to 2047 stands exactly once in the table. Each run of 64 page ids that starts at a multiple of 64 holds at least one page of every prefix.
All inputs are finite; a program needn't handle non-finite values. No bound on the sum of `suffix_lens` on one device may be relied on, other than what follows from the above.
Results may differ from the reference program's by a relative error of at most 0.005.
Values may be sent and summed in bfloat16 or wider, within the bound.
A program may use at most 192 MiB of HBM per device.

```python
import math
import jax
import jax.numpy as jnp
import numpy as np
from jax import lax

H = 32
KV = 8
HD = 128
NPREF = 2
PAGE = 16
PAGES_DEV = 64
B_DEV = 16
SUF = 256
B = 512
PAGES = 2048
PPP = 1024
N_SEQ = 32


def shared_keys(key):
    raw_keys = 4.0 * jax.random.normal(jax.random.fold_in(key, 11), (B, KV * HD), jnp.float32)
    return jnp.clip(raw_keys, -24.0, 24.0)


def draw_new_keys(key, part):
    return shared_keys(key).astype(jnp.bfloat16)


def draw_queries(key, part):
    plain_draw = jnp.clip(jax.random.normal(jax.random.fold_in(key, 12), (B, H * HD), jnp.float32), -6.0, 6.0)
    return plain_draw.astype(jnp.bfloat16)


def draw_page_table(key, part):
    owner_count = PAGES // PAGES_DEV
    spare_slots = PAGES_DEV - NPREF
    leftover = jnp.repeat(jnp.arange(NPREF, dtype=jnp.int32), PPP - owner_count)
    leftover = jax.random.permutation(jax.random.fold_in(key, 3), leftover).reshape(owner_count, spare_slots)
    base_rows = jnp.tile(jnp.arange(NPREF, dtype=jnp.int32)[None, :], (owner_count, 1))
    labels = jnp.concatenate([base_rows, leftover], axis=1)
    labels = jax.random.permutation(jax.random.fold_in(key, 4), labels, axis=1, independent=True)
    order_list = jnp.argsort(labels.reshape(-1), stable=True)
    return order_list.reshape(NPREF, PPP).astype(jnp.int32)


def set_ends(drawn, stream_key, smallest, high):
    dims = drawn.shape
    spot = [jax.random.randint(jax.random.fold_in(stream_key, axis), (), 0, dims[axis]) for axis in range(len(dims))]
    drawn = drawn.at[tuple(spot)].set(smallest)
    longest = dims.index(max(dims))
    spot[longest] = (spot[longest] + 1) % dims[longest]
    return drawn.at[tuple(spot)].set(high)


def block_levels(key, dims, cuts, least, high):
    loudness, own = 1.0, jax.random.fold_in(key, 6)
    for dim, parts in cuts:
        draws = jnp.exp(jax.random.uniform(jax.random.fold_in(own, dim), (parts,), jnp.float32, least / len(cuts), high / len(cuts)))
        loudness = loudness * jnp.repeat(draws, dims[dim] // parts).reshape([-1 if axis == dim else 1 for axis in range(len(dims))])
    return loudness


def rank_bounds(number_of, skew):
    loads = [(1 << 20) // math.isqrt(standing ** skew) + 1 for standing in range(1, number_of + 1)]
    deviation = 1 + sum(loads) // (1 << 30)
    return np.cumsum(np.array([max(1, weight // deviation) for weight in loads]))


def ranked_ids(rng, extent, count, skew):
    table = rank_bounds(count, skew)
    lot = jax.random.randint(jax.random.fold_in(rng, 1), extent, 0, int(table[count - 1]))
    rank = jnp.searchsorted(jnp.asarray(table, jnp.int32), lot, side="right")
    return jax.random.permutation(jax.random.fold_in(rng, 2), count)[rank].astype(jnp.int32)


def split_up(count, total, most, skew):
    loads = [(1 << 20) // math.isqrt(standing ** skew) + 1 for standing in range(2, count + 1)]
    spare, counts = total - most - (count - 1), [1] * (count - 1)
    while spare > 0:
        free = [i for i in range(count - 1) if counts[i] < most]
        whole, remaining = sum([loads[i] for i in free]), spare
        for i in free:
            extra = min(most - counts[i], max(1, remaining * loads[i] // whole), spare)
            counts[i] = counts[i] + extra
            spare = spare - extra
    return np.array([most] + counts)


def ragged_sizes(key, count, total, reach, lean):
    if count == 2:
        one = jax.random.randint(key, (), max(1, total - reach), min(reach, total - 1) + 1)
        return jnp.stack([one, total - one])
    tallies = jnp.asarray(split_up(count, total, reach, lean), jnp.int32)
    couples = (count - 1) // 2
    source_of, taker = tallies[1:1 + 2 * couples:2], tallies[2:2 + 2 * couples:2]
    room = jnp.minimum(source_of - 1, reach - taker)
    shifted = jax.random.randint(jax.random.fold_in(key, 1), (couples,), 0, 1 << 20) % (room + 1)
    tallies = tallies.at[1:1 + 2 * couples:2].set(source_of - shifted).at[2:2 + 2 * couples:2].set(taker + shifted)
    return tallies[jax.random.permutation(jax.random.fold_in(key, 2), count)]


def gaussian(rng, dims, width, limit, pieces=(), kind=jnp.bfloat16):
    array = jax.random.normal(rng, dims, jnp.float32) * width
    if len(pieces) > 0:
        array = block_levels(rng, dims, pieces, -0.22, 0.18) * array
    return jnp.clip(array, min=-limit, max=limit).astype(kind)


def setup_inputs(seed: int = 0, part: int = 0) -> dict:
    key_list = jax.random.split(jax.random.key(seed), 11)
    part_splits = jax.random.split(jax.random.fold_in(key_list[10], part), 11)
    return {
        "queries": draw_queries(jax.random.fold_in(jax.random.fold_in(key_list[10], part), 71), part),
        "new_keys": draw_new_keys(jax.random.fold_in(jax.random.fold_in(key_list[10], part), 71), part),
        "new_values": gaussian(part_splits[2], (B, KV * HD), 2.0, 12.0, ((0, 32),)),
        "suffix_keys": gaussian(part_splits[3], (B, SUF, KV * HD), 3.0, 18.0, ((0, 32),)),
        "suffix_values": gaussian(part_splits[4], (B, SUF, KV * HD), 2.0, 12.0, ((0, 32),)),
        "suffix_lens": ragged_sizes(part_splits[5], B, B * SUF // 2, SUF, 2).astype(jnp.int32),
        "prefix_keys": gaussian(part_splits[6], (PAGES, PAGE, KV * HD), 2.0, 12.0, ((0, 32),)),
        "prefix_values": gaussian(part_splits[7], (PAGES, PAGE, KV * HD), 2.0, 12.0, ((0, 32),)),
        "page_table": draw_page_table(jax.random.fold_in(jax.random.fold_in(key_list[10], part), 71), part),
        "prefix_id": set_ends(ranked_ids(part_splits[9], (B,), NPREF, 2), jax.random.fold_in(part_splits[9], 3), 0, NPREF - 1).astype(jnp.int32),
    }


def reference(queries, new_keys, new_values, suffix_keys, suffix_values, suffix_lens, prefix_keys, prefix_values, page_table, prefix_id):
    group_size = H // KV
    softmax_scale = 1.0 / math.sqrt(HD)
    block_tokens = PAGES_DEV * PAGE
    page_ids = jnp.arange(PAGES, dtype=jnp.int32)
    page_hits = jnp.any(page_table[:, :, None] == page_ids[None, None, :], axis=1)
    prefix_of_page = lax.optimization_barrier(jnp.sum(page_hits.astype(jnp.int32) * jnp.arange(NPREF, dtype=jnp.int32)[:, None], axis=0))
    token_label = jnp.repeat(prefix_of_page, PAGE)
    pool_keys = prefix_keys.reshape(PAGES * PAGE, KV, HD).astype(jnp.float32)
    pool_values = prefix_values.reshape(N_SEQ, block_tokens, KV, HD).astype(jnp.float32)
    block_count = B // B_DEV
    slot_index = jnp.arange(SUF, dtype=jnp.int32)

    def one_block(inputs):
        block_queries, block_new_keys, block_new_values, block_suffix_keys, block_suffix_values, block_lens, block_ids = inputs
        query_head_count = block_queries.reshape(B_DEV, KV, group_size, HD).astype(jnp.float32)
        prefix_scores = jnp.einsum('bkgd,tkd->bkgt', query_head_count, pool_keys) * softmax_scale
        prefix_live = (block_ids[:, None] == token_label[None, :])[:, None, None, :]
        prefix_scores = jnp.where(prefix_live, prefix_scores, -1e+30)
        prefix_scores = prefix_scores.reshape(B_DEV, KV, group_size, N_SEQ, block_tokens)
        prefix_live = prefix_live.reshape(B_DEV, 1, 1, N_SEQ, block_tokens)
        block_peak = lax.optimization_barrier(jnp.max(prefix_scores, axis=4))
        block_weights = jnp.where(prefix_live, jnp.exp(prefix_scores - block_peak[..., None]), 0.0)
        block_mass = lax.optimization_barrier(jnp.sum(block_weights, axis=4))
        block_round = lax.optimization_barrier(block_weights.astype(jnp.bfloat16)).astype(jnp.float32)
        block_numer = jnp.einsum('bkgot,otkd->bkgod', block_round, pool_values)
        block_out = block_numer / block_mass[..., None]
        block_out = lax.optimization_barrier(block_out.astype(jnp.bfloat16)).astype(jnp.float32)
        block_lse = block_peak + jnp.log(block_mass)
        own_keys = block_suffix_keys.reshape(B_DEV, SUF, KV, HD).astype(jnp.float32)
        own_values = block_suffix_values.reshape(B_DEV, SUF, KV, HD).astype(jnp.float32)
        suffix_scores = jnp.einsum('bkgd,btkd->bkgt', query_head_count, own_keys) * softmax_scale
        suffix_live = (slot_index[None, :] < block_lens[:, None])[:, None, None, :]
        suffix_scores = jnp.where(suffix_live, suffix_scores, -1e+30)
        incoming_keys = block_new_keys.reshape(B_DEV, KV, HD).astype(jnp.float32)
        incoming_values = block_new_values.reshape(B_DEV, KV, HD).astype(jnp.float32)
        incoming_scores = jnp.einsum('iqnc,iqc->iqn', query_head_count, incoming_keys) * softmax_scale
        home_peak = jnp.maximum(lax.optimization_barrier(jnp.max(suffix_scores, axis=3)), incoming_scores)
        suffix_weights = jnp.where(suffix_live, jnp.exp(suffix_scores - home_peak[..., None]), 0.0)
        fresh_weights = jnp.exp(incoming_scores - home_peak)
        home_mass = lax.optimization_barrier(jnp.sum(suffix_weights, axis=3)) + fresh_weights
        suffix_round = lax.optimization_barrier(suffix_weights.astype(jnp.bfloat16)).astype(jnp.float32)
        incoming_rounded = lax.optimization_barrier(fresh_weights.astype(jnp.bfloat16)).astype(jnp.float32)
        resident_numerator = jnp.einsum('bkgt,btkd->bkgd', suffix_round, own_values)
        resident_numerator = resident_numerator + jnp.einsum('cqx,cqh->cqxh', incoming_rounded, incoming_values)
        home_out = resident_numerator / home_mass[..., None]
        home_lse = home_peak + jnp.log(home_mass)
        overall = jnp.maximum(lax.optimization_barrier(jnp.max(block_lse, axis=3)), home_lse)
        factor = jnp.exp(block_lse - overall[..., None])
        home_factor = jnp.exp(home_lse - overall)
        merged = lax.optimization_barrier(jnp.sum(factor[..., None] * block_out, axis=3)) + home_factor[..., None] * home_out
        divisor = lax.optimization_barrier(jnp.sum(factor, axis=3)) + home_factor
        result = merged / divisor[..., None]
        return result.reshape(B_DEV, H * HD).astype(jnp.bfloat16)
    stacked = (queries.reshape(block_count, B_DEV, H * HD), new_keys.reshape(block_count, B_DEV, KV * HD), new_values.reshape(block_count, B_DEV, KV * HD), suffix_keys.reshape(block_count, B_DEV, SUF, KV * HD), suffix_values.reshape(block_count, B_DEV, SUF, KV * HD), suffix_lens.reshape(block_count, B_DEV), prefix_id.reshape(block_count, B_DEV))
    outputs = lax.map(one_block, stacked)
    return outputs.reshape(B, H * HD)
```

```python
import functools
import math

import jax
import jax.numpy as jnp
from jax import lax
from jax.experimental import pallas as pl
from jax.experimental.pallas import tpu as pltpu
from jax.sharding import PartitionSpec as P

KV = 8
HD = 128
NPREF = 2
CORES = 2
PARTS = 4
LOW = -1e30
MESH = pl.DeviceIdType.MESH
F32 = jnp.float32
BF16 = jnp.bfloat16


def kernel(
    chips,
    c2,
    q_hbm,
    nk_ref,
    nv_ref,
    ks_hbm,
    vs_hbm,
    lens_ref,
    pk_hbm,
    pv_hbm,
    pen_ref,
    oh_ref,
    out_ref,
    qr,
    qp,
    kraw,
    vraw,
    kt,
    va,
    ko,
    vo,
    own,
    psend,
    precv,
    lown,
    lpsend,
    lprecv,
    rs,
    rss,
    rsd,
    rsds,
    qh,
    ho,
    hl,
    nk32,
    nv32,
    loc_sem,
    suf_sem,
    ring_send,
    ring_recv,
    qp_send,
    qp_recv,
    p_send,
    p_recv,
    ps_send,
    ps_recv,
    rs_send,
    rs_recv,
    rss_send,
    rss_recv,
):
    far = chips // 2
    rows = q_hbm.shape[0]
    width = q_hbm.shape[1] // PARTS
    heads = q_hbm.shape[1] // HD
    part_heads = heads // PARTS
    group = heads // KV
    part_kv = KV // PARTS
    half = rows // 2
    slots = ks_hbm.shape[1]

    me = lax.axis_index("seq")
    z, core = me // CORES, me % CORES
    right = {"seq": ((z + 1) % chips) * CORES + core}
    left = {"seq": ((z + chips - 1) % chips) * CORES + core}
    mate = {"seq": z * CORES + (1 - core)}

    def remote(src, dst, send, recv, device):
        return pltpu.make_async_remote_copy(
            src_ref=src, dst_ref=dst, send_sem=send, recv_sem=recv, device_id=device, device_id_type=MESH
        )

    q_in = [
        pltpu.make_async_copy(q_hbm.at[:, pl.ds(s * width, width)], qr.at[far - 1, s, 1], loc_sem.at[s])
        for s in range(PARTS)
    ]
    k_in = pltpu.make_async_copy(pk_hbm, kraw, loc_sem.at[PARTS])
    v_in = pltpu.make_async_copy(pv_hbm, vraw, loc_sem.at[PARTS + 1])
    for copy in q_in:
        copy.start()
    k_in.start()
    v_in.start()

    def suffix_copies(b):
        return (
            pltpu.make_async_copy(ks_hbm.at[b], ko.at[b], suf_sem.at[0, b]),
            pltpu.make_async_copy(vs_hbm.at[b], vo.at[b], suf_sem.at[1, b]),
        )

    barrier = pltpu.get_barrier_semaphore()
    for device in (left, right, mate):
        pl.semaphore_signal(barrier, inc=1, device_id=device, device_id_type=MESH)
    pl.semaphore_wait(barrier, 3)

    def ring_copy(direction, source, slot, s):
        return remote(
            source,
            qr.at[slot, s, direction],
            ring_send.at[direction, s],
            ring_recv.at[direction, slot, s],
            right if direction == 0 else left,
        )

    def mate_queries(slot, s):
        return remote(qr.at[slot, s], qp.at[slot, s], qp_send.at[s], qp_recv.at[slot, s], mate)

    def mate_partial(slot, s):
        return remote(psend.at[slot, s], precv.at[slot, s], p_send.at[s], p_recv.at[slot, s], mate)

    def mate_stats(slot):
        return remote(lpsend.at[slot], lprecv.at[slot], ps_send, ps_recv.at[slot], mate)

    for s in range(PARTS):
        q_in[s].wait()
        for direction in (0, 1):
            ring_copy(direction, qr.at[far - 1, s, 1], 0, s).start()

    @pl.loop(0, rows)
    def _(b):
        for copy in suffix_copies(b):
            copy.start()

    lown[...] = jnp.zeros_like(lown)
    lpsend[...] = jnp.zeros_like(lpsend)
    for direction, k in ((0, far + 1), (1, far), (1, far + 1)):
        rs[direction, k] = jnp.zeros(rs.shape[2:], rs.dtype)
        rss[direction, k] = jnp.full(rss.shape[2:], LOW, F32)

    k_in.wait()

    @pl.loop(0, KV)
    def _(h):
        columns = pl.ds(pl.multiple_of(h * HD, HD), HD)
        kt[h, 0:HD, :] = kraw[:, columns].T
        kt[h, HD:, :] = pen_ref[...]

    v_in.wait()

    @pl.loop(0, KV)
    def _(h):
        columns = pl.ds(pl.multiple_of(h * HD, HD), HD)
        va[h, :, 0:HD] = vraw[:, columns]
        va[h, :, HD:] = jnp.ones((va.shape[1], HD), BF16)

    for s in range(PARTS):
        for i in range(part_heads):
            qh[pl.ds(s * part_heads + i, rows, stride=heads), :] = qr[far - 1, s, 1, :, i * HD : (i + 1) * HD].astype(F32)
    nk32[...] = nk_ref[...].astype(F32)
    nv32[...] = nv_ref[...].astype(F32)

    lane = lax.broadcasted_iota(jnp.int32, (half, HD), 1)

    def attend(slot, s):
        k = slot + 1
        chip_of = ((z + chips - k) % chips, jnp.where(k == far, z, (z + k) % chips))
        onehots = [oh_ref[chip_of[d] * CORES + (core if src == 0 else 1 - core)] for src in (0, 1) for d in (0, 1)]
        stats = [lown[slot, 0], lown[slot, 1], lpsend[slot, 0], lpsend[slot, 1]]
        for i in range(part_kv):
            h = s * part_kv + i
            tiles = []
            for src, ref in enumerate((qr, qp)):
                for d in (0, 1):
                    for g in range(group):
                        at = (i * group + g) * HD
                        tiles.append(jnp.concatenate([ref[slot, s, d, :, at : at + HD], onehots[src * 2 + d]], axis=1))
            qa = jnp.concatenate(tiles, axis=0)
            score = jnp.dot(qa, kt[h], preferred_element_type=F32)
            peak = jnp.max(score, axis=1, keepdims=True)
            weight = jnp.exp2((score - peak) * c2).astype(BF16)
            summed = jnp.dot(weight, va[h], preferred_element_type=F32)
            mass = summed[:, HD:]
            part = summed[:, :HD] / mass
            lse = peak * c2 + jnp.log2(mass)
            for src in (0, 1):
                for d in (0, 1):
                    for g in range(group):
                        row = ((src * 2 + d) * group + g) * rows
                        at = (i * group + g) * HD
                        tile = part[row : row + rows]
                        if src == 0:
                            own[slot, s, d, :, at : at + HD] = tile
                        else:
                            psend[slot, s, d, :, at : at + HD] = tile.astype(BF16)
                        head = s * part_heads + i * group + g
                        n = src * 2 + d
                        stats[n] = jnp.where(lane == head, lse[row : row + half], stats[n])
                        stats[n] = jnp.where(lane == head + heads, lse[row + half : row + rows], stats[n])
        lown[slot, 0], lown[slot, 1], lpsend[slot, 0], lpsend[slot, 1] = stats

    def attend_and_send(slot, s):
        mate_queries(slot, s).wait_recv()
        attend(slot, s)

        @pl.when(slot >= 1)
        def _():
            mate_partial(slot, s).wait_send()

        mate_partial(slot, s).start()

        @pl.when(s == PARTS - 1)
        def _():
            @pl.when(slot >= 1)
            def _():
                mate_stats(slot).wait_send()

            mate_stats(slot).start()

    @pl.loop(0, far * PARTS)
    def _(step):
        slot, s = step // PARTS, step % PARTS
        ring_copy(0, qr.at[slot, s, 0], slot, s).wait_recv()

        @pl.when(slot < far - 1)
        def _():
            onward = ring_copy(0, qr.at[slot, s, 0], slot + 1, s)
            onward.wait_send()
            onward.start()
            ring_copy(1, qr.at[slot, s, 1], slot, s).wait_recv()

        @pl.when(slot < far - 2)
        def _():
            onward = ring_copy(1, qr.at[slot, s, 1], slot + 1, s)
            onward.wait_send()
            onward.start()

        @pl.when(slot >= 1)
        def _():
            mate_queries(slot, s).wait_send()

        mate_queries(slot, s).start()

        @pl.when(step >= 1)
        def _():
            attend_and_send((step - 1) // PARTS, (step - 1) % PARTS)

    attend_and_send(far - 1, PARTS - 1)

    for s in range(PARTS):
        ring_copy(0, qr.at[0, s, 0], 0, s).wait_send()
        ring_copy(1, qr.at[0, s, 1], 0, s).wait_send()
        mate_queries(0, s).wait_send()
        mate_partial(0, s).wait_send()
    mate_stats(0).wait_send()

    def stat_copy(direction, k):
        return remote(
            rsds.at[direction, k],
            rss.at[direction, k],
            rss_send.at[direction],
            rss_recv.at[direction, k],
            left if direction == 0 else right,
        )

    def part_copy(direction, k, s):
        return remote(
            rsd.at[direction, k, s],
            rs.at[direction, k, s],
            rs_send.at[direction, s],
            rs_recv.at[direction, k, s],
            left if direction == 0 else right,
        )

    def across(tile, i):
        low = jnp.broadcast_to(tile[:, i : i + 1], (half, HD))
        high = jnp.broadcast_to(tile[:, heads + i : heads + i + 1], (half, HD))
        return jnp.concatenate([low, high], axis=0)

    def shares(stats):
        top = functools.reduce(jnp.maximum, stats)
        total = top + jnp.log2(sum(jnp.exp2(s - top) for s in stats))
        return total, [jnp.exp2(s - total) for s in stats[1:]]

    row_of = lax.broadcasted_iota(jnp.int32, (heads, KV * HD), 0)
    col_of = lax.broadcasted_iota(jnp.int32, (heads, KV * HD), 1)
    sub = lax.broadcasted_iota(jnp.int32, (2 * group, HD), 0)

    def home(b):
        for copy in suffix_copies(b):
            copy.wait()
        at = pl.ds(pl.multiple_of(b * heads, heads), heads)
        wide = jnp.concatenate([qh[at, :]] * KV, axis=1)
        wide = jnp.where(row_of // group == col_of // HD, wide, 0.0)
        score = lax.dot_general(
            wide.astype(BF16), ko[b], (((1,), (1,)), ((), ())), preferred_element_type=F32
        )
        slot_of = lax.broadcasted_iota(jnp.int32, (heads, slots), 1)
        score = jnp.where(slot_of < lens_ref[b], score, LOW)
        fresh = jnp.sum(wide * nk32[pl.ds(b, 1), :], axis=1, keepdims=True)
        peak = jnp.maximum(jnp.max(score, axis=1, keepdims=True), fresh)
        weight = jnp.exp2((score - peak) * c2)
        fresh = jnp.exp2((fresh - peak) * c2)
        mass = jnp.sum(weight, axis=1, keepdims=True) + fresh
        summed = jnp.dot(weight.astype(BF16), vo[b], preferred_element_type=F32)
        summed = summed + fresh.astype(BF16).astype(F32) * nv32[pl.ds(b, 1), :]
        picked = []
        for i in range(KV // 2):
            r = slice(2 * i * group, 2 * (i + 1) * group)
            first = summed[r, 2 * i * HD : (2 * i + 1) * HD]
            second = summed[r, (2 * i + 1) * HD : (2 * i + 2) * HD]
            picked.append(jnp.where(sub < group, first, second))
        ho[at, :] = jnp.concatenate(picked, axis=0) / mass
        hl[at, :] = jnp.broadcast_to(peak * c2 + jnp.log2(mass), (heads, HD))

    per_step = -(-rows // far)

    @pl.loop(0, far)
    def _(j):
        k = far - j
        slot = k - 1
        mate_stats(slot).wait_recv()

        @pl.when(k < far)
        def _():
            stat_copy(0, k + 1).wait_recv()

        @pl.when(k < far - 1)
        def _():
            stat_copy(1, k + 1).wait_recv()

        factors = []
        for d in (0, 1):
            total, weights = shares([lown[slot, d], lprecv[slot, d], rss[d, k + 1]])
            rsds[d, k] = total
            factors.append(weights)

        @pl.when(k < far)
        def _():
            stat_copy(0, k).wait_send()

        stat_copy(0, k).start()

        @pl.when(k < far - 1)
        def _():
            stat_copy(1, k).wait_send()

        @pl.when(k < far)
        def _():
            stat_copy(1, k).start()

        for s in range(PARTS):
            mate_partial(slot, s).wait_recv()

            @pl.when(k < far)
            def _():
                part_copy(0, k + 1, s).wait_recv()

            @pl.when(k < far - 1)
            def _():
                part_copy(1, k + 1, s).wait_recv()

            for d in (0, 1):
                for i in range(part_heads):
                    at = slice(i * HD, (i + 1) * HD)
                    head = s * part_heads + i
                    mine = own[slot, s, d, :, at]
                    merged = mine + across(factors[d][0], head) * (precv[slot, s, d, :, at].astype(F32) - mine)
                    merged = merged + across(factors[d][1], head) * (rs[d, k + 1, s, :, at].astype(F32) - mine)
                    rsd[d, k, s, :, at] = merged.astype(BF16)

                if d == 0:

                    @pl.when(k < far)
                    def _():
                        part_copy(0, k, s).wait_send()

                    part_copy(0, k, s).start()
                else:

                    @pl.when(k < far - 1)
                    def _():
                        part_copy(1, k, s).wait_send()

                    @pl.when(k < far)
                    def _():
                        part_copy(1, k, s).start()

        for n in range(per_step):
            b = j * per_step + n

            @pl.when(b < rows)
            def _():
                home(b)

    for d in (0, 1):
        stat_copy(d, 1).wait_recv()
    total, weights = shares([lown[far - 1, 1], lprecv[far - 1, 1], rss[0, 1], rss[1, 1]])
    for s in range(PARTS):
        for d in (0, 1):
            part_copy(d, 1, s).wait_recv()
        for i in range(part_heads):
            at = slice(i * HD, (i + 1) * HD)
            head = s * part_heads + i
            mine = own[far - 1, s, 1, :, at]
            merged = mine + across(weights[0], head) * (precv[far - 1, s, 1, :, at].astype(F32) - mine)
            merged = merged + across(weights[1], head) * (rs[0, 1, s, :, at].astype(F32) - mine)
            merged = merged + across(weights[2], head) * (rs[1, 1, s, :, at].astype(F32) - mine)
            home_lse = hl[pl.ds(head, rows, stride=heads), :]
            home_out = ho[pl.ds(head, rows, stride=heads), :]
            share = 1.0 / (1.0 + jnp.exp2(across(total, head) - home_lse))
            merged = merged + share * (home_out - merged)
            out_ref[:, s * width + i * HD : s * width + (i + 1) * HD] = merged.astype(BF16)

    for d in (0, 1):
        stat_copy(d, 1).wait_send()
        for s in range(PARTS):
            part_copy(d, 1, s).wait_send()


def local(
    queries,
    new_keys,
    new_values,
    suffix_keys,
    suffix_values,
    suffix_lens,
    prefix_keys,
    prefix_values,
    page_table,
    prefix_id,
):
    devices = lax.axis_size("seq")
    chips = devices // CORES
    far = chips // 2
    rows, columns = queries.shape
    width = columns // PARTS
    heads = columns // HD
    pages, page, kv_columns = prefix_keys.shape
    tokens = pages * page
    slots = suffix_keys.shape[1]
    half = rows // 2

    ids = lax.axis_index("seq") * pages + jnp.arange(pages, dtype=jnp.int32)
    held = jnp.any(page_table[:, :, None] == ids[None, None, :], axis=1)
    penalty = jnp.where(held, 0.0, LOW).astype(BF16)
    penalty = jnp.repeat(penalty, page, axis=1)
    penalty = jnp.concatenate([penalty, jnp.zeros((HD - NPREF, tokens), BF16)], axis=0)
    onehot = (prefix_id[:, None] == jnp.arange(HD, dtype=jnp.int32)[None, :]).astype(BF16)
    onehot = onehot.reshape(devices, rows, HD)

    any_space = pl.BlockSpec(memory_space=pl.ANY)
    vmem = pl.BlockSpec(memory_space=pltpu.VMEM)
    smem = pl.BlockSpec(memory_space=pltpu.SMEM)
    dma = pltpu.SemaphoreType.DMA
    chunk = (PARTS, 2, rows, width)
    return pl.pallas_call(
        functools.partial(kernel, chips, math.log2(math.e) / math.sqrt(HD)),
        out_shape=jax.ShapeDtypeStruct((rows, columns), BF16),
        in_specs=[any_space, vmem, vmem, any_space, any_space, smem, any_space, any_space, vmem, vmem],
        out_specs=vmem,
        scratch_shapes=[
            pltpu.VMEM((far, *chunk), BF16),
            pltpu.VMEM((far, *chunk), BF16),
            pltpu.VMEM((tokens, kv_columns), BF16),
            pltpu.VMEM((tokens, kv_columns), BF16),
            pltpu.VMEM((KV, 2 * HD, tokens), BF16),
            pltpu.VMEM((KV, tokens, 2 * HD), BF16),
            pltpu.VMEM((rows, slots, kv_columns), BF16),
            pltpu.VMEM((rows, slots, kv_columns), BF16),
            pltpu.VMEM((far, *chunk), F32),
            pltpu.VMEM((far, *chunk), BF16),
            pltpu.VMEM((far, *chunk), BF16),
            pltpu.VMEM((far, 2, half, HD), F32),
            pltpu.VMEM((far, 2, half, HD), F32),
            pltpu.VMEM((far, 2, half, HD), F32),
            pltpu.VMEM((2, far + 2, PARTS, rows, width), BF16),
            pltpu.VMEM((2, far + 2, half, HD), F32),
            pltpu.VMEM((2, far + 1, PARTS, rows, width), BF16),
            pltpu.VMEM((2, far + 1, half, HD), F32),
            pltpu.VMEM((rows * heads, HD), F32),
            pltpu.VMEM((rows * heads, HD), F32),
            pltpu.VMEM((rows * heads, HD), F32),
            pltpu.VMEM((rows, kv_columns), F32),
            pltpu.VMEM((rows, kv_columns), F32),
            dma((PARTS + 2,)),
            dma((2, rows)),
            dma((2, PARTS)),
            dma((2, far, PARTS)),
            dma((PARTS,)),
            dma((far, PARTS)),
            dma((PARTS,)),
            dma((far, PARTS)),
            dma,
            dma((far,)),
            dma((2, PARTS)),
            dma((2, far + 2, PARTS)),
            dma((2,)),
            dma((2, far + 2)),
        ],
        compiler_params=pltpu.CompilerParams(
            collective_id=0, has_side_effects=True, vmem_limit_bytes=64000000
        ),
    )(
        queries,
        new_keys,
        new_values,
        suffix_keys,
        suffix_values,
        suffix_lens,
        prefix_keys.reshape(tokens, kv_columns),
        prefix_values.reshape(tokens, kv_columns),
        penalty,
        onehot,
    )


def solution(mesh):
    spread = ("grp", "seq")
    placed = (
        P(spread, None),
        P(spread, None),
        P(spread, None),
        P(spread, None, None),
        P(spread, None, None),
        P(spread),
        P(spread, None, None),
        P(spread, None, None),
        P("grp", None),
        P("grp"),
    )
    return jax.shard_map(local, mesh=mesh, in_specs=placed, out_specs=P(spread, None), check_vma=False)
```

```python
import functools
import math

import jax
import jax.numpy as jnp
from jax import lax
from jax.experimental import pallas as pl
from jax.experimental.pallas import tpu as pltpu
from jax.sharding import PartitionSpec as P

KV = 8
HD = 128
NPREF = 2
CORES = 2
PARTS = 4
HALF = PARTS // 2
LOW = -1e30
MESH = pl.DeviceIdType.MESH
F32 = jnp.float32
BF16 = jnp.bfloat16


def kernel(
    chips,
    c2,
    page_size,
    q_hbm,
    nk_ref,
    nv_ref,
    ks_hbm,
    vs_hbm,
    lens_ref,
    pk_hbm,
    pv_hbm,
    table_ref,
    pid_ref,
    out_ref,
    qr,
    qp,
    kraw,
    vraw,
    kt,
    oh,
    even,
    odd,
    weight_of,
    va,
    ko,
    vo,
    own,
    psend,
    precv,
    lown,
    lpsend,
    lprecv,
    rs,
    rss,
    rsd,
    rsds,
    qh,
    ho,
    hl,
    nk32,
    nv32,
    loc_sem,
    suf_sem,
    ring_send,
    ring_recv,
    qp_send,
    qp_recv,
    p_send,
    p_recv,
    ps_send,
    ps_recv,
    rs_send,
    rs_recv,
    rss_send,
    rss_recv,
):
    far = chips // 2
    rows = q_hbm.shape[0]
    width = q_hbm.shape[1] // PARTS
    heads = q_hbm.shape[1] // HD
    part_heads = heads // PARTS
    group = heads // KV
    part_kv = KV // PARTS
    half = rows // 2
    slots = ks_hbm.shape[1]
    pages = kraw.shape[0] // page_size

    me = lax.axis_index("seq")
    z, core = me // CORES, me % CORES
    right = {"seq": ((z + 1) % chips) * CORES + 1 - core}
    left = {"seq": ((z + chips - 1) % chips) * CORES + 1 - core}
    mate = {"seq": z * CORES + (1 - core)}

    def remote(src, dst, send, recv, device):
        return pltpu.make_async_remote_copy(
            src_ref=src, dst_ref=dst, send_sem=send, recv_sem=recv, device_id=device, device_id_type=MESH
        )

    q_in = [
        pltpu.make_async_copy(q_hbm.at[:, pl.ds(s * width, width)], qr.at[far - 1, s, 1], loc_sem.at[s])
        for s in range(PARTS)
    ]
    k_in = pltpu.make_async_copy(pk_hbm, kraw, loc_sem.at[PARTS])
    v_in = pltpu.make_async_copy(pv_hbm, vraw, loc_sem.at[PARTS + 1])
    for copy in q_in:
        copy.start()
    k_in.start()
    v_in.start()

    def suffix_copies(b):
        return (
            pltpu.make_async_copy(ks_hbm.at[b], ko.at[b], suf_sem.at[0, b]),
            pltpu.make_async_copy(vs_hbm.at[b], vo.at[b], suf_sem.at[1, b]),
        )

    barrier = pltpu.get_barrier_semaphore()
    for device in (left, right, mate):
        pl.semaphore_signal(barrier, inc=1, device_id=device, device_id_type=MESH)
    pl.semaphore_wait(barrier, 3)

    def ring_copy(direction, source, slot, s):
        return remote(
            source,
            qr.at[slot, s, direction],
            ring_send.at[direction, s],
            ring_recv.at[direction, slot, s],
            right if direction == 0 else left,
        )

    def mate_queries(slot, s):
        return remote(qr.at[slot, s], qp.at[slot, s], qp_send.at[s], qp_recv.at[slot, s], mate)

    def mate_partial(slot, s):
        return remote(psend.at[slot, s], precv.at[slot, s], p_send.at[s], p_recv.at[slot, s], mate)

    def mate_stats(slot):
        return remote(lpsend.at[slot], lprecv.at[slot], ps_send, ps_recv.at[slot], mate)

    for s in range(PARTS):
        q_in[s].wait()
        for direction in (0, 1):
            ring_copy(direction, qr.at[far - 1, s, 1], 0, s).start()

    lown[...] = jnp.zeros_like(lown)
    lpsend[...] = jnp.zeros_like(lpsend)
    for d in (0, 1):
        rs[d, far + 1] = jnp.zeros(rs.shape[2:], rs.dtype)
        rss[d, far + 1] = jnp.full(rss.shape[2:], LOW, F32)
        for s in range(PARTS):
            if s // HALF != d:
                rs[d, far, s] = jnp.zeros(rs.shape[3:], rs.dtype)

    tokens = kraw.shape[0]
    mine_of = me * pages + lax.broadcasted_iota(jnp.int32, (pages, table_ref.shape[1]), 0)
    column = lax.broadcasted_iota(jnp.int32, (pages, HD), 1)
    missing = jnp.zeros((pages, HD), F32)
    for p in range(NPREF):
        hit = jnp.where(table_ref[p : p + 1, :] == mine_of, 1.0, 0.0)
        hit = jnp.max(hit, axis=1, keepdims=True)
        missing = jnp.where(column == p, 1.0 - hit, missing)
    page_of = lax.broadcasted_iota(jnp.int32, (pages, tokens), 1) // page_size
    spread = jnp.where(page_of == lax.broadcasted_iota(jnp.int32, (pages, tokens), 0), 1.0, 0.0).astype(BF16)
    penalty = jnp.dot(missing.T.astype(BF16), spread, preferred_element_type=F32)
    penalty = jnp.where(penalty > 0.5, LOW, 0.0).astype(BF16)

    ids = pid_ref[...].astype(F32)
    ids = jnp.concatenate([ids, jnp.zeros((HD - ids.shape[0], HD), F32)], axis=0).T
    choice = lax.broadcasted_iota(jnp.int32, (HD, HD), 1).astype(F32)
    for n in range(pid_ref.shape[0]):
        flags = jnp.where(choice == jnp.broadcast_to(ids[:, n : n + 1], (HD, HD)), 1.0, 0.0)
        oh[n * HD : (n + 1) * HD, :] = flags.astype(BF16)

    k_in.wait()

    @pl.loop(0, KV)
    def _(h):
        columns = pl.ds(pl.multiple_of(h * HD, HD), HD)
        kt[h, 0:HD, :] = kraw[:, columns].T
        kt[h, HD:, :] = penalty

    v_in.wait()

    @pl.loop(0, KV)
    def _(h):
        columns = pl.ds(pl.multiple_of(h * HD, HD), HD)
        va[h, :, 0:HD] = vraw[:, columns]
        va[h, :, HD:] = jnp.ones((va.shape[1], HD), BF16)

    @pl.loop(0, rows)
    def _(b):
        for copy in suffix_copies(b):
            copy.start()

    for s in range(PARTS):
        for i in range(part_heads):
            qh[pl.ds(s * part_heads + i, rows, stride=heads), :] = qr[far - 1, s, 1, :, i * HD : (i + 1) * HD].astype(F32)
    nk32[...] = nk_ref[...].astype(F32)
    nv32[...] = nv_ref[...].astype(F32)

    lane = lax.broadcasted_iota(jnp.int32, (half, HD), 1)

    def score_into(step, score):
        slot, s = step // PARTS, step % PARTS
        k = slot + 1
        chip_of = ((z + chips - k) % chips, jnp.where(k == far, z, (z + k) % chips))
        came = [(core + k) % CORES, jnp.where(k == far, core, (core + k) % CORES)]
        onehots = []
        for src in (0, 1):
            for d in (0, 1):
                device = chip_of[d] * CORES + (came[d] if src == 0 else 1 - came[d])
                onehots.append(oh[pl.ds(pl.multiple_of(device * rows, rows), rows), :])
        for i in range(part_kv):
            tiles = []
            for src, ref in enumerate((qr, qp)):
                for d in (0, 1):
                    for g in range(group):
                        at = (i * group + g) * HD
                        tiles.append(jnp.concatenate([ref[slot, s, d, :, at : at + HD], onehots[src * 2 + d]], axis=1))
            score[i] = jnp.dot(jnp.concatenate(tiles, axis=0), kt[s * part_kv + i], preferred_element_type=F32)

    def weigh(step, score):
        slot, s = step // PARTS, step % PARTS
        stats = [lown[slot, 0], lown[slot, 1], lpsend[slot, 0], lpsend[slot, 1]]
        peaks = [jnp.max(score[i], axis=1, keepdims=True) for i in range(part_kv)]
        for i in range(part_kv):
            weight_of[i] = jnp.exp2((score[i] - peaks[i]) * c2).astype(BF16)
        sums = [jnp.dot(weight_of[i], va[s * part_kv + i], preferred_element_type=F32) for i in range(part_kv)]
        for i in range(part_kv):
            mass = sums[i][:, HD:]
            part = sums[i][:, :HD] / mass
            lse = peaks[i] * c2 + jnp.log2(mass)
            for src in (0, 1):
                for d in (0, 1):
                    for g in range(group):
                        row = ((src * 2 + d) * group + g) * rows
                        at = (i * group + g) * HD
                        tile = part[row : row + rows]
                        if src == 0:
                            own[slot, s, d, :, at : at + HD] = tile
                        else:
                            psend[slot, s, d, :, at : at + HD] = tile.astype(BF16)
                        head = s * part_heads + i * group + g
                        n = src * 2 + d
                        stats[n] = jnp.where(lane == head, lse[row : row + half], stats[n])
                        stats[n] = jnp.where(lane == head + heads, lse[row + half : row + rows], stats[n])
        lown[slot, 0], lown[slot, 1], lpsend[slot, 0], lpsend[slot, 1] = stats

    def send_partial(step):
        slot, s = step // PARTS, step % PARTS

        @pl.when(slot >= 1)
        def _():
            mate_partial(slot, s).wait_send()

        mate_partial(slot, s).start()

        @pl.when(s == PARTS - 1)
        def _():
            @pl.when(slot >= 1)
            def _():
                mate_stats(slot).wait_send()

            mate_stats(slot).start()

    def far_copy(direction, source, s):
        return remote(
            source,
            qr.at[far - 1, s, 0],
            ring_send.at[direction, s],
            ring_recv.at[direction, far - 1, s],
            right if direction == 0 else left,
        )

    def forward(step):
        slot, s = step // PARTS, step % PARTS
        for d in (0, 1):
            carries = s // HALF == d

            @pl.when(slot < far - 1)
            def _():
                ring_copy(d, qr.at[slot, s, d], slot, s).wait_recv()

            @pl.when(slot < far - 2)
            def _():
                onward = ring_copy(d, qr.at[slot, s, d], slot + 1, s)
                onward.wait_send()
                onward.start()

            @pl.when((slot == far - 2) & carries)
            def _():
                onward = far_copy(d, qr.at[slot, s, d], s)
                onward.wait_send()
                onward.start()

            @pl.when((slot == far - 1) & carries)
            def _():
                far_copy(d, qr.at[0, s, d], s).wait_recv()

        @pl.when(slot >= 1)
        def _():
            mate_queries(slot, s).wait_send()

        mate_queries(slot, s).start()

    def advance(step, into, ready):
        mate_queries((step - 1) // PARTS, (step - 1) % PARTS).wait_recv()
        score_into(step - 1, into)
        weigh(jnp.maximum(step - 2, 0), ready)

        @pl.when(step >= 2)
        def _():
            send_partial(step - 2)

    @pl.loop(0, far * PARTS // 2)
    def _(pair):
        forward(2 * pair)

        @pl.when(pair >= 1)
        def _():
            advance(2 * pair, odd, even)

        forward(2 * pair + 1)
        advance(2 * pair + 1, even, odd)

    last = jnp.int32(far * PARTS)
    advance(last, odd, even)
    weigh(last - 1, odd)
    send_partial(last - 1)

    for s in range(PARTS):
        ring_copy(0, qr.at[0, s, 0], 0, s).wait_send()
        ring_copy(1, qr.at[0, s, 1], 0, s).wait_send()
        mate_queries(0, s).wait_send()
        mate_partial(0, s).wait_send()
    mate_stats(0).wait_send()

    def stat_copy(direction, k):
        return remote(
            rsds.at[direction, k],
            rss.at[direction, k],
            rss_send.at[direction],
            rss_recv.at[direction, k],
            left if direction == 0 else right,
        )

    def part_copy(direction, k, s):
        return remote(
            rsd.at[direction, k, s],
            rs.at[direction, k, s],
            rs_send.at[direction, s],
            rs_recv.at[direction, k, s],
            left if direction == 0 else right,
        )

    def across(tile, i):
        low = jnp.broadcast_to(tile[:, i : i + 1], (half, HD))
        high = jnp.broadcast_to(tile[:, heads + i : heads + i + 1], (half, HD))
        return jnp.concatenate([low, high], axis=0)

    def shares(stats):
        top = functools.reduce(jnp.maximum, stats)
        total = top + jnp.log2(sum(jnp.exp2(s - top) for s in stats))
        return total, [jnp.exp2(s - total) for s in stats[1:]]

    row_of = lax.broadcasted_iota(jnp.int32, (heads, KV * HD), 0)
    col_of = lax.broadcasted_iota(jnp.int32, (heads, KV * HD), 1)
    sub = lax.broadcasted_iota(jnp.int32, (2 * group, HD), 0)

    def home(b):
        for copy in suffix_copies(b):
            copy.wait()
        at = pl.ds(pl.multiple_of(b * heads, heads), heads)
        wide = jnp.concatenate([qh[at, :]] * KV, axis=1)
        wide = jnp.where(row_of // group == col_of // HD, wide, 0.0)
        score = lax.dot_general(
            wide.astype(BF16), ko[b], (((1,), (1,)), ((), ())), preferred_element_type=F32
        )
        slot_of = lax.broadcasted_iota(jnp.int32, (heads, slots), 1)
        score = jnp.where(slot_of < lens_ref[b], score, LOW)
        fresh = jnp.sum(wide * nk32[pl.ds(b, 1), :], axis=1, keepdims=True)
        peak = jnp.maximum(jnp.max(score, axis=1, keepdims=True), fresh)
        weight = jnp.exp2((score - peak) * c2)
        fresh = jnp.exp2((fresh - peak) * c2)
        mass = jnp.sum(weight, axis=1, keepdims=True) + fresh
        summed = jnp.dot(weight.astype(BF16), vo[b], preferred_element_type=F32)
        summed = summed + fresh.astype(BF16).astype(F32) * nv32[pl.ds(b, 1), :]
        picked = []
        for i in range(KV // 2):
            r = slice(2 * i * group, 2 * (i + 1) * group)
            first = summed[r, 2 * i * HD : (2 * i + 1) * HD]
            second = summed[r, (2 * i + 1) * HD : (2 * i + 2) * HD]
            picked.append(jnp.where(sub < group, first, second))
        ho[at, :] = jnp.concatenate(picked, axis=0) / mass
        hl[at, :] = jnp.broadcast_to(peak * c2 + jnp.log2(mass), (heads, HD))

    per_step = -(-rows // far)

    part_half = lane % heads // (HALF * part_heads)

    @pl.loop(0, far)
    def _(j):
        k = far - j
        slot = k - 1
        mate_stats(slot).wait_recv()

        @pl.when(k < far)
        def _():
            for d in (0, 1):
                stat_copy(d, k + 1).wait_recv()

        factors = []
        side = [jnp.where(k == far, 0, d) for d in (0, 1)]
        for d in (0, 1):
            total, weights = shares([lown[slot, side[d]], lprecv[slot, side[d]], rss[d, k + 1]])
            rsds[d, k] = jnp.where((part_half == d) | (k < far), total, LOW)
            factors.append(weights)
        for d in (0, 1):

            @pl.when(k < far)
            def _():
                stat_copy(d, k).wait_send()

            stat_copy(d, k).start()

        for n in range(PARTS):
            for d in (0, 1):
                s = (n + d * HALF) % PARTS
                carries = s // HALF == d
                if n < HALF:
                    mate_partial(slot, s).wait_recv()

                @pl.when(k < (far if carries else far - 1))
                def _():
                    part_copy(d, k + 1, s).wait_recv()

                for i in range(part_heads):
                    at = slice(i * HD, (i + 1) * HD)
                    head = s * part_heads + i
                    mine = own[slot, s, side[d], :, at]
                    merged = mine + across(factors[d][0], head) * (precv[slot, s, side[d], :, at].astype(F32) - mine)
                    merged = merged + across(factors[d][1], head) * (rs[d, k + 1, s, :, at].astype(F32) - mine)
                    rsd[d, k, s, :, at] = merged.astype(BF16)

                @pl.when(k < (far if carries else far - 1))
                def _():
                    part_copy(d, k, s).wait_send()

                if carries:
                    part_copy(d, k, s).start()
                else:

                    @pl.when(k < far)
                    def _():
                        part_copy(d, k, s).start()

        for n in range(per_step):
            b = j * per_step + n

            @pl.when(b < rows)
            def _():
                home(b)

    home_stats = jnp.zeros((half, HD), F32)
    for head in range(heads):
        tile = hl[pl.ds(head, rows, stride=heads), :]
        home_stats = jnp.where(lane == head, tile[:half], home_stats)
        home_stats = jnp.where(lane == head + heads, tile[half:], home_stats)
    base, weights = shares([lown[far - 1, 1], lprecv[far - 1, 1], home_stats])
    for s in range(PARTS):
        for i in range(part_heads):
            at = slice(i * HD, (i + 1) * HD)
            head = s * part_heads + i
            mine = own[far - 1, s, 1, :, at]
            merged = mine + across(weights[0], head) * (precv[far - 1, s, 1, :, at].astype(F32) - mine)
            merged = merged + across(weights[1], head) * (ho[pl.ds(head, rows, stride=heads), :] - mine)
            own[far - 1, s, 1, :, at] = merged

    for d in (0, 1):
        stat_copy(d, 1).wait_recv()
    total, weights = shares([base, rss[0, 1], rss[1, 1]])
    for s in range(PARTS):
        for d in (0, 1):
            part_copy(d, 1, s).wait_recv()
        for i in range(part_heads):
            at = slice(i * HD, (i + 1) * HD)
            head = s * part_heads + i
            mine = own[far - 1, s, 1, :, at]
            merged = mine + across(weights[0], head) * (rs[0, 1, s, :, at].astype(F32) - mine)
            merged = merged + across(weights[1], head) * (rs[1, 1, s, :, at].astype(F32) - mine)
            out_ref[:, s * width + i * HD : s * width + (i + 1) * HD] = merged.astype(BF16)

    for d in (0, 1):
        stat_copy(d, 1).wait_send()
        for s in range(PARTS):
            part_copy(d, 1, s).wait_send()


def local(
    queries,
    new_keys,
    new_values,
    suffix_keys,
    suffix_values,
    suffix_lens,
    prefix_keys,
    prefix_values,
    page_table,
    prefix_id,
):
    devices = lax.axis_size("seq")
    chips = devices // CORES
    far = chips // 2
    rows, columns = queries.shape
    width = columns // PARTS
    heads = columns // HD
    pages, page, kv_columns = prefix_keys.shape
    tokens = pages * page
    slots = suffix_keys.shape[1]
    half = rows // 2

    any_space = pl.BlockSpec(memory_space=pl.ANY)
    vmem = pl.BlockSpec(memory_space=pltpu.VMEM)
    smem = pl.BlockSpec(memory_space=pltpu.SMEM)
    dma = pltpu.SemaphoreType.DMA
    chunk = (PARTS, 2, rows, width)
    return pl.pallas_call(
        functools.partial(kernel, chips, math.log2(math.e) / math.sqrt(HD), page),
        out_shape=jax.ShapeDtypeStruct((rows, columns), BF16),
        in_specs=[any_space, vmem, vmem, any_space, any_space, smem, any_space, any_space, vmem, vmem],
        out_specs=vmem,
        scratch_shapes=[
            pltpu.VMEM((far, *chunk), BF16),
            pltpu.VMEM((far, *chunk), BF16),
            pltpu.VMEM((tokens, kv_columns), BF16),
            pltpu.VMEM((tokens, kv_columns), BF16),
            pltpu.VMEM((KV, 2 * HD, tokens), BF16),
            pltpu.VMEM((devices * rows, HD), BF16),
            pltpu.VMEM((KV // PARTS, 4 * (heads // KV) * rows, tokens), F32),
            pltpu.VMEM((KV // PARTS, 4 * (heads // KV) * rows, tokens), F32),
            pltpu.VMEM((KV // PARTS, 4 * (heads // KV) * rows, tokens), BF16),
            pltpu.VMEM((KV, tokens, 2 * HD), BF16),
            pltpu.VMEM((rows, slots, kv_columns), BF16),
            pltpu.VMEM((rows, slots, kv_columns), BF16),
            pltpu.VMEM((far, *chunk), F32),
            pltpu.VMEM((far, *chunk), BF16),
            pltpu.VMEM((far, *chunk), BF16),
            pltpu.VMEM((far, 2, half, HD), F32),
            pltpu.VMEM((far, 2, half, HD), F32),
            pltpu.VMEM((far, 2, half, HD), F32),
            pltpu.VMEM((2, far + 2, PARTS, rows, width), BF16),
            pltpu.VMEM((2, far + 2, half, HD), F32),
            pltpu.VMEM((2, far + 1, PARTS, rows, width), BF16),
            pltpu.VMEM((2, far + 1, half, HD), F32),
            pltpu.VMEM((rows * heads, HD), F32),
            pltpu.VMEM((rows * heads, HD), F32),
            pltpu.VMEM((rows * heads, HD), F32),
            pltpu.VMEM((rows, kv_columns), F32),
            pltpu.VMEM((rows, kv_columns), F32),
            dma((PARTS + 2,)),
            dma((2, rows)),
            dma((2, PARTS)),
            dma((2, far, PARTS)),
            dma((PARTS,)),
            dma((far, PARTS)),
            dma((PARTS,)),
            dma((far, PARTS)),
            dma,
            dma((far,)),
            dma((2, PARTS)),
            dma((2, far + 2, PARTS)),
            dma((2,)),
            dma((2, far + 2)),
        ],
        compiler_params=pltpu.CompilerParams(
            collective_id=0, has_side_effects=True, vmem_limit_bytes=64000000
        ),
    )(
        queries,
        new_keys,
        new_values,
        suffix_keys,
        suffix_values,
        suffix_lens,
        prefix_keys.reshape(tokens, kv_columns),
        prefix_values.reshape(tokens, kv_columns),
        page_table,
        prefix_id.reshape(-1, HD),
    )


def solution(mesh):
    spread = ("grp", "seq")
    placed = (
        P(spread, None),
        P(spread, None),
        P(spread, None),
        P(spread, None, None),
        P(spread, None, None),
        P(spread),
        P(spread, None, None),
        P(spread, None, None),
        P("grp", None),
        P("grp"),
    )
    return jax.shard_map(local, mesh=mesh, in_specs=placed, out_specs=P(spread, None), check_vma=False)
```
